512 devices in a mesh: row: 32 (over z, x_hi, core), col: 16 (over y, x_lo).
Axes of the slice: x: 4 (x_hi: 2, x_lo: 2; x = x_hi * 2 + x_lo), y: 8, z: 8, core: 2. Of those that a mesh axis runs over, the one named last changes fastest.
Arguments:
- ancestor: float32 [32, 384, 12288], P(None, 'col', 'row'), may hold values from -6 to 6
- panels: float32 [2, 12288, 512], P(None, ('row', 'col')), may hold values from -0.06 to 0.06
- link_panels: float32 [1, 512, 512], P(None, 'row'), may hold values from -0.25 to 0.25
- diag_inverse: float32 [2, 512, 512], P(None, 'row'), may hold values from -0.25 to 0.25
- blocks: int32 [2, 48], replicated, may hold values from 0 to 95, as said below
Outputs:
- columns: float32 [2, 12288, 512], P(None, ('row', 'col'))
- diagonal: float32 [2, 512, 512], P(None, 'row', 'col')
The draws below stay inside these ranges and needn't reach their ends.
Inputs may be any that keep to these rules, and one draw needn't show every extreme that they name: Each of the 2 rows names 48 different row blocks.
All inputs are finite; a program needn't handle non-finite values.
Results may differ from the reference program's by a relative error of at most 0.0001.
Values sent between devices are 32-bit elements; how exact they have to be, the bound alone decides.
A program may use at most 64 MiB of HBM per device.

```python
import jax
import jax.numpy as jnp
from jax import lax

M = 12288
W = 512
BLOCK = 128
NSUP = 2
SEL = 48
N_ROW = 32


def draw_blocks(key, part):
    rows_list = [jax.random.permutation(jax.random.fold_in(key, 17 + number), M // BLOCK)[:SEL] for number in range(NSUP)]
    return jnp.stack(rows_list).astype(jnp.int32)


def levels(key, shape, split, least, top_value):
    def one(dim, blocks):
        draws = jax.random.uniform(jax.random.fold_in(jax.random.fold_in(key, 6), dim), (blocks,), jnp.float32, least / len(split), top_value / len(split))
        return jnp.repeat(jnp.exp(draws), shape[dim] // blocks).reshape((-1,) + (1,) * (len(shape) - dim - 1))

    factor_of = one(*split[0])
    for cut in split[1:]:
        factor_of = factor_of * one(*cut)
    return factor_of


def normal_values(rng, dims, scale, reach, cuts=(), kind=jnp.bfloat16):
    loudness = levels(rng, dims, cuts, -0.22, 0.18) if cuts else 1.0
    result = jax.random.normal(rng, dims, jnp.float32) * scale * loudness
    return jnp.minimum(jnp.maximum(result, -reach), reach).astype(kind)


def setup_inputs(seed: int = 0) -> dict:
    streams_of = jax.random.split(jax.random.key(seed), 6)
    return {
        "ancestor": normal_values(streams_of[0], (N_ROW, M // N_ROW, M), 1.0, 6.0, ((1, 16), (2, 32)), jnp.float32),
        "panels": normal_values(streams_of[1], (NSUP, M, W), 0.01, 0.06, ((1, 512),), jnp.float32),
        "link_panels": normal_values(streams_of[2], (NSUP - 1, W, W), W ** -0.5, 0.25, ((1, 32),), jnp.float32),
        "diag_inverse": normal_values(streams_of[3], (NSUP, W, W), W ** -0.5, 0.25, ((1, 32),), jnp.float32),
        "blocks": draw_blocks(jax.random.fold_in(streams_of[5], 71), 0),
    }


def matmul(left, right):
    return jnp.dot(left, right, precision=lax.Precision.HIGHEST, preferred_element_type=jnp.float32)


def reference(ancestor, panels, link_panels, diag_inverse, blocks):
    whole = ancestor.reshape(M, M).T
    row_block = jnp.arange(M, dtype=jnp.int32) // BLOCK
    positions = jnp.arange(W, dtype=jnp.int32)
    lower_mask = positions[None, :] <= positions[:, None]
    col_list = []
    diag_list = []
    prev_cols = None
    prev_diag = None
    for supernode in range(NSUP):
        chosen = jnp.any(row_block[:, None] == blocks[supernode][None, :], axis=1)
        panel = jnp.where(chosen[:, None], panels[supernode], jnp.float32(0.0))
        product = matmul(whole, panel)
        lowered = jnp.where(lower_mask, diag_inverse[supernode], jnp.float32(0.0))
        gram = matmul(lowered.T, lowered)
        if supernode == 0:
            cols_now = -product
            diag_now = gram - matmul(panel.T, cols_now)
        else:
            link = link_panels[supernode - 1]
            carried = matmul(prev_cols, link)
            cols_now = -(product + carried)
            diag_now = gram - matmul(panel.T, cols_now) + matmul(carried.T, panel) + matmul(link.T, matmul(prev_diag, link))
        col_list.append(cols_now)
        diag_list.append(diag_now)
        prev_cols = cols_now
        prev_diag = diag_now
    return jnp.stack(col_list), jnp.stack(diag_list)
```

```python
import jax
import jax.numpy as jnp
from jax import lax
from jax.experimental import pallas as pl
from jax.experimental.pallas import tpu as pltpu
from jax.sharding import PartitionSpec as P

BLOCK = 128
F32 = jnp.float32
BF16 = jnp.bfloat16
MESH = pl.DeviceIdType.MESH


def halves_of(value):
    high = value.astype(BF16)
    return high, (value - high.astype(F32)).astype(BF16)


def dot(left, right):
    return jnp.dot(left, right, preferred_element_type=F32)


def dot3(lh, ll, rh, rl):
    return dot(lh, rh) + (dot(lh, rl) + dot(ll, rh))


def kernel(
    pay, anc, low, cols, diag,
    pbuf, ebuf, ehi, elo, fbuf, xa, sap, sam, rap, ram, sbp, sbm, rbp, rbm, xbs, xb,
    bhi, blo, prh, prl, ssend, sbuf, dsend, dbuf, tsend, tbuf, gsend, gbuf,
    esem, ag_s, ag_r, rs_s, rs_r, ex_s, ex_r,
):
    r = lax.axis_index("row")
    c = lax.axis_index("col")
    z, xh, k = r // 4, (r // 2) % 2, r % 2
    y, xl = c // 2, c % 2
    kk = r // 2

    def at_row(zz, hh, co):
        return (lax.rem(zz + 8, 8) * 4 + hh * 2 + co, c)

    def at_col(yy, ll):
        return (r, lax.rem(yy + 8, 8) * 2 + ll)

    zp, zm = at_row(z + 1, xh, k), at_row(z - 1, xh, k)
    xpart, cpart = at_row(z, 1 - xh, k), at_row(z, xh, 1 - k)
    yp, ym, lpart = at_col(y + 1, xl), at_col(y - 1, xl), at_col(y, 1 - xl)

    fetch = pltpu.make_async_copy(anc, ebuf, esem)
    fetch.start()

    barrier = pltpu.get_barrier_semaphore()
    near = (zp, zm, xpart, cpart, yp, ym, lpart)
    for peer in near:
        pl.semaphore_signal(barrier, inc=1, device_id=peer, device_id_type=MESH)
    pl.semaphore_wait(barrier, len(near))

    sends = []

    def remote(src, dst, ss, rs, to):
        return pltpu.make_async_remote_copy(
            src_ref=src, dst_ref=dst, send_sem=ss, recv_sem=rs, device_id=to, device_id_type=MESH
        )

    def chip(zz, hh):
        return lax.rem(zz + 8, 8) * 2 + hh

    ring = {}

    def ag(name, src, block, to):
        n = len(ring)
        ring[name] = remote(src, pbuf.at[block, k], ag_s.at[n], ag_r.at[n], to)
        ring[name].start()
        sends.append(ring[name])

    def arrived(name, block):
        ring[name].wait_recv()
        return pbuf.at[block, k]

    mine = chip(z, xh)
    other = chip(z, 1 - xh)
    ag("x", pay, mine, xpart)
    ag("po0", pay, mine, zp)
    ag("mo0", pay, mine, zm)
    ag("cx", pay, mine, cpart)
    pbuf[mine, k] = pay[...]

    fetch.wait()
    for i in range(6):
        h, l = halves_of(ebuf[i * 128 : (i + 1) * 128, :].T)
        ehi[:, i * 128 : (i + 1) * 128] = h
        elo[:, i * 128 : (i + 1) * 128] = l

    src = arrived("x", other)
    ag("pp0", src, other, zp)
    ag("mp0", src, other, zm)
    ag("cp", src, other, cpart)
    for s in range(4):
        for tag, sign, hh, last in (("po", -1, xh, 3), ("mo", 1, xh, 2), ("pp", -1, 1 - xh, 2), ("mp", 1, 1 - xh, 3)):
            if s > last:
                continue
            block = chip(z + sign * (s + 1), hh)
            src = arrived(f"{tag}{s}", block)
            if s < last:
                ag(f"{tag}{s + 1}", src, block, zp if sign < 0 else zm)
            ag(f"c{tag}{s}", src, block, cpart)
    for name in list(ring):
        if name[0] == "c":
            ring[name].wait_recv()

    rsn = []

    def rs(src, dst, to):
        n = len(rsn)
        copy = remote(src, dst, rs_s.at[n], rs_r.at[n], to)
        rsn.append(copy)
        sends.append(copy)
        copy.start()
        return copy

    def product(half):
        def step(n, _):
            at = pl.ds(pl.multiple_of(half * 512 + n * 256, 256), 256)
            ph, plo = halves_of(pbuf[:, :, 0:24, at].reshape(768, 256))
            fbuf[:, :, :, at] = dot3(ehi[...], elo[...], ph, plo).reshape(8, 2, 24, 256)
            return 0

        lax.fori_loop(0, 2, step, 0)

    def yy(d):
        return lax.rem(y + d + 8, 8)

    A, B = pl.ds(0, 512), pl.ds(512, 512)
    product(0)
    xac = {}
    for d in (4, 3, -3, 2, -2, 1, -1, 0):
        xac[d] = rs(fbuf.at[yy(d), 1 - xl, :, A], xa.at[yy(d)], lpart)
    product(1)
    bp = [rs(fbuf.at[yy(3), :, :, B], rbp.at[0], yp)]
    bm = [rs(fbuf.at[yy(-4), :, :, B], rbm.at[0], ym)]

    for g in range(4):
        part = pbuf[g * 4 : g * 4 + 4, :, 24:32, :].reshape(8, 8, 1024)
        rows = jnp.concatenate([part[:, :, 0:512], part[:, :, 512:1024]], axis=1).reshape(128, 512)
        h, l = halves_of(rows)
        bhi[g * 128 : (g + 1) * 128, :] = h
        blo[g * 128 : (g + 1) * 128, :] = l
    for g in range(2):
        h, l = halves_of(pbuf[g * 8 : g * 8 + 8, pl.ds(k, 1), 0:24, :].reshape(192, 1024))
        rows = slice(g * 192, (g + 1) * 192)
        prh[rows, 0:1024] = h
        prl[rows, 0:1024] = l
        rh, rl = halves_of(dot3(h[:, 0:512], l[:, 0:512], bhi[...], blo[...]))
        prh[rows, 1024:1536] = rh
        prl[rows, 1024:1536] = rl
    lane = lax.broadcasted_iota(jnp.int32, (1, 128), 1)
    l0 = low[0]
    l1 = low[1]
    h, l = halves_of(l0)
    m0 = dot3(h, l, bhi[...], blo[...])
    gsend[0:16, 0:512] = l0
    gsend[16:32, 0:512] = l1
    gsend[32:48, 0:512] = m0
    chunk = gsend[0:48, pl.ds(pl.multiple_of((c // 4) * 128, 128), 128)]
    off = lax.rem(c, 4) * 32
    to0 = pltpu.roll(chunk, lax.rem(128 - off, 128), 1)
    to1 = pltpu.roll(chunk, lax.rem(160 - off, 128), 1)
    row = lax.broadcasted_iota(jnp.int32, (48, 128), 0)
    wide = jnp.where(row < 16, jnp.where(lane < 32, to0, 0.0), jnp.where((lane >= 32) & (lane < 64), to1, 0.0))
    wide = wide + pltpu.roll(wide, 64, 1)
    ut = jnp.concatenate([gsend[0:48, 0:512], jnp.zeros((80, 512), F32)], axis=0).T
    wide = jnp.concatenate([wide, jnp.zeros((80, 128), F32)], axis=0)
    uh, ul = halves_of(ut)
    wh, wl = halves_of(wide)
    gpart = dot3(uh, ul, wh, wl).reshape(32, 2, 8, 128)
    gbuf[0] = jnp.where(lane < 64, gpart[:, 0], gpart[:, 1])

    def send_g(i, _):
        to = lax.rem(r + i, 32)
        remote(gbuf.at[0, to], gbuf.at[1, r], ex_s.at[0], ex_r.at[0], (to, c)).start()
        return 0

    lax.fori_loop(1, 32, send_g, 0)
    gbuf[1, r] = gbuf[0, r]

    xac[4].wait_recv()
    sap[0] = fbuf[yy(4), xl, :, A] + xa[yy(4)]
    ap = [rs(sap.at[0], rap.at[0], yp)]
    am = []
    for s in range(1, 4):
        if s < 3:
            bp[s - 1].wait_recv()
            sbp[s] = fbuf[yy(3 - s), :, :, B] + rbp[s - 1]
            bp.append(rs(sbp.at[s], rbp.at[s], yp))
        bm[s - 1].wait_recv()
        sbm[s] = fbuf[yy(s - 4), :, :, B] + rbm[s - 1]
        bm.append(rs(sbm.at[s], rbm.at[s], ym))
        xac[4 - s].wait_recv()
        ap[s - 1].wait_recv()
        sap[s] = fbuf[yy(4 - s), xl, :, A] + xa[yy(4 - s)] + rap[s - 1]
        ap.append(rs(sap.at[s], rap.at[s], yp))
        xac[s - 4].wait_recv()
        if s == 1:
            sam[0] = fbuf[yy(-3), xl, :, A] + xa[yy(-3)]
        else:
            am[s - 2].wait_recv()
            sam[s - 1] = fbuf[yy(s - 4), xl, :, A] + xa[yy(s - 4)] + ram[s - 2]
        am.append(rs(sam.at[s - 1], ram.at[s - 1], ym))
    bp[2].wait_recv()
    bm[3].wait_recv()
    xbs[...] = fbuf[y, :, :, B] + rbp[2] + rbm[3]
    xbc = rs(xbs.at[1 - xl], xb, lpart)
    xac[0].wait_recv()
    ap[3].wait_recv()
    am[2].wait_recv()
    c0 = -(fbuf[y, xl, :, A] + xa[y] + rap[3] + ram[2])
    h, l = halves_of(c0)
    carried = dot3(h, l, bhi[...], blo[...])
    xbc.wait_recv()
    c1 = -(xbs[xl] + xb[...] + carried)
    cols[0] = c0
    cols[1] = c1

    for q in range(16):
        at = slice((q // 4) * 128, (q // 4) * 128 + 128)
        o = (q % 4) * 32

        def turned(value, place):
            shift = (place - o) % 128
            return value if shift == 0 else pltpu.roll(value, shift, 1)

        ssend[q] = jnp.where(
            lane < 32,
            turned(c0[:, at], 0),
            jnp.where(lane < 64, turned(c1[:, at], 32), jnp.where(lane < 96, turned(carried[:, at], 64), 0.0)),
        )

    def send_s(i, _):
        to = lax.rem(kk + i, 16)
        remote(ssend.at[to], sbuf.at[kk], ex_s.at[1], ex_r.at[1], (to * 2 + k, c)).start()
        return 0

    lax.fori_loop(1, 16, send_s, 0)
    sbuf[kk] = ssend[kk]

    def settle(buf, count, sem):
        pltpu.make_async_copy(buf.at[pl.ds(0, count)], buf.at[pl.ds(0, count)], sem).wait()

    settle(sbuf, 15, ex_r.at[1])
    h, l = halves_of(sbuf[...].reshape(384, 128).T)
    out = dot3(h, l, prh[...], prl[...])
    d0 = -out[0:32, 0:512]
    d1 = -(out[32:64, 512:1024] + out[64:96, 1024:1536])
    dt = jnp.concatenate([d0, d1, d0, d1], axis=0).T.reshape(32, 2, 8, 128)
    dsend[...] = jnp.where(lane < 64, dt[:, 0], dt[:, 1])
    tt = out[64:96, 512:1024].reshape(2, 2, 8, 512)
    for q in range(16):
        at = slice((q // 4) * 128, (q // 4) * 128 + 128)
        o = (q % 4) * 32
        for half in range(2):
            first, second = tt[half, 0, :, at], tt[half, 1, :, at]
            s1, s2 = (32 - o) % 128, (96 - o) % 128
            first = first if s1 == 0 else pltpu.roll(first, s1, 1)
            second = second if s2 == 0 else pltpu.roll(second, s2, 1)
            tsend[q * 2 + half] = jnp.where(
                lane >= 96, second, jnp.where((lane >= 32) & (lane < 64), first, 0.0)
            )
    slot = c * 2 + k

    def send_d(i, _):
        to = lax.rem(r + i, 32)
        remote(dsend.at[to], dbuf.at[slot], ex_s.at[2], ex_r.at[2], (to, kk)).start()
        return 0

    def send_t(i, _):
        to = lax.rem(slot + i, 32)
        remote(tsend.at[to], tbuf.at[slot], ex_s.at[3], ex_r.at[3], (kk * 2 + lax.rem(to, 2), to // 2)).start()
        return 0

    lax.fori_loop(1, 32, send_d, 0)
    inside = kk == c

    @pl.when(inside)
    def _():
        dbuf[slot] = dsend[r]

    @pl.when(jnp.logical_not(inside))
    def _():
        remote(dsend.at[r], dbuf.at[slot], ex_s.at[4], ex_r.at[2], (r, kk)).start()

    lax.fori_loop(1, 32, send_t, 0)
    tbuf[slot] = tsend[slot]

    settle(gbuf.at[1], 31, ex_r.at[0])
    total = jnp.sum(gbuf[1], axis=0)
    settle(tbuf, 31, ex_r.at[3])
    total = total + jnp.sum(tbuf[...], axis=0)

    @pl.when(inside)
    def _():
        settle(dbuf, 31, ex_r.at[2])

    @pl.when(jnp.logical_not(inside))
    def _():
        settle(dbuf, 32, ex_r.at[2])
        settle(dsend, 1, ex_s.at[4])

    total = total + jnp.sum(dbuf[...], axis=0)
    diag[0, 0:8, :] = total[:, 0:32]
    diag[1, 0:8, :] = pltpu.roll(total, 96, 1)[:, 0:32]
    diag[0, 8:16, :] = pltpu.roll(total, 64, 1)[:, 0:32]
    diag[1, 8:16, :] = pltpu.roll(total, 32, 1)[:, 0:32]

    settle(gbuf.at[1], 31, ex_s.at[0])
    settle(sbuf, 15, ex_s.at[1])
    settle(dbuf, 31, ex_s.at[2])
    settle(tbuf, 31, ex_s.at[3])
    for copy in sends:
        copy.wait_send()


def body(ancestor, panels, link_panels, diag_inverse, blocks):
    r = lax.axis_index("row")
    c = lax.axis_index("col")
    resident = ancestor.reshape(768, 384)
    first = (r * 16 + c) * 24
    row_block = (first + jnp.arange(24, dtype=jnp.int32)) // BLOCK
    hit = jnp.any(row_block[None, :, None] == blocks[:, None, :], axis=2)
    masked = jnp.where(hit[:, :, None], panels, jnp.float32(0.0))
    link = link_panels[0]
    pay = jnp.concatenate(
        [
            jnp.concatenate([masked[0], masked[1]], axis=1),
            jnp.concatenate([link[0:8], link[8:16]], axis=1),
        ],
        axis=0,
    )
    rows = r * 16 + jnp.arange(16, dtype=jnp.int32)
    keep = jnp.arange(512, dtype=jnp.int32)[None, :] <= rows[:, None]
    low = jnp.where(keep[None], diag_inverse, jnp.float32(0.0))
    vmem = pl.BlockSpec(memory_space=pltpu.VMEM)
    return pl.pallas_call(
        kernel,
        out_shape=(
            jax.ShapeDtypeStruct((2, 24, 512), F32),
            jax.ShapeDtypeStruct((2, 16, 32), F32),
        ),
        in_specs=[vmem, pl.BlockSpec(memory_space=pl.ANY), vmem],
        out_specs=(vmem, vmem),
        scratch_shapes=[
            pltpu.VMEM((16, 2, 32, 1024), F32),
            pltpu.VMEM((768, 384), F32),
            pltpu.VMEM((384, 768), BF16),
            pltpu.VMEM((384, 768), BF16),
            pltpu.VMEM((8, 2, 24, 1024), F32),
            pltpu.VMEM((8, 24, 512), F32),
            pltpu.VMEM((4, 24, 512), F32),
            pltpu.VMEM((3, 24, 512), F32),
            pltpu.VMEM((4, 24, 512), F32),
            pltpu.VMEM((3, 24, 512), F32),
            pltpu.VMEM((3, 2, 24, 512), F32),
            pltpu.VMEM((4, 2, 24, 512), F32),
            pltpu.VMEM((3, 2, 24, 512), F32),
            pltpu.VMEM((4, 2, 24, 512), F32),
            pltpu.VMEM((2, 24, 512), F32),
            pltpu.VMEM((24, 512), F32),
            pltpu.VMEM((512, 512), BF16),
            pltpu.VMEM((512, 512), BF16),
            pltpu.VMEM((384, 1536), BF16),
            pltpu.VMEM((384, 1536), BF16),
            pltpu.VMEM((16, 24, 128), F32),
            pltpu.VMEM((16, 24, 128), F32),
            pltpu.VMEM((32, 8, 128), F32),
            pltpu.VMEM((32, 8, 128), F32),
            pltpu.VMEM((32, 8, 128), F32),
            pltpu.VMEM((32, 8, 128), F32),
            pltpu.VMEM((48, 512), F32),
            pltpu.VMEM((2, 32, 8, 128), F32),
            pltpu.SemaphoreType.DMA,
            pltpu.SemaphoreType.DMA((31,)),
            pltpu.SemaphoreType.DMA((31,)),
            pltpu.SemaphoreType.DMA((23,)),
            pltpu.SemaphoreType.DMA((23,)),
            pltpu.SemaphoreType.DMA((5,)),
            pltpu.SemaphoreType.DMA((4,)),
        ],
        compiler_params=pltpu.CompilerParams(
            collective_id=0, has_side_effects=True, vmem_limit_bytes=40 * 1024 * 1024
        ),
    )(pay, resident, low)


def solution(mesh):
    return jax.shard_map(
        body,
        mesh=mesh,
        in_specs=(
            P(None, "col", "row"),
            P(None, ("row", "col"), None),
            P(None, "row", None),
            P(None, "row", None),
            P(),
        ),
        out_specs=(P(None, ("row", "col"), None), P(None, "row", "col")),
        check_vma=False,
    )
```

```python
import jax
import jax.numpy as jnp
from jax import lax
from jax.experimental import pallas as pl
from jax.experimental.pallas import tpu as pltpu
from jax.sharding import PartitionSpec as P

BLOCK = 128
F32 = jnp.float32
BF16 = jnp.bfloat16
MESH = pl.DeviceIdType.MESH


def halves_of(value):
    high = value.astype(BF16)
    return high, (value - high.astype(F32)).astype(BF16)


def dot(left, right):
    return jnp.dot(left, right, preferred_element_type=F32)


def dot3(lh, ll, rh, rl):
    return dot(lh, rh) + (dot(lh, rl) + dot(ll, rh))


def turned(value, shift):
    shift = shift % 128
    return value if shift == 0 else pltpu.roll(value, shift, 1)


def kernel(
    anc, pan, lnk, inv, blk, cols, diag,
    pb0, pb1, bb, praw, low, hits, ebuf, ehi, elo, f0, f1, xa, sbuf, rbuf,
    bhi, blo, prh, prl, s0send, s0buf, s1send, s1buf, dsend, dbuf, tsend, tbuf, gsend, gbuf,
    in_s, ag_s, ag_r, rs_s, rs_r, ex_s, ex_r,
):
    r = lax.axis_index("row")
    c = lax.axis_index("col")
    z, xh, k = r // 4, (r // 2) % 2, r % 2
    y, xl = c // 2, c % 2
    kk = r // 2
    lane = lax.broadcasted_iota(jnp.int32, (1, 128), 1)

    def wrap(i):
        return lax.rem(i + 8, 8)

    def at_row(zz, hh, co):
        return (wrap(zz) * 4 + hh * 2 + co, c)

    def at_col(yy, ll):
        return (r, wrap(yy) * 2 + ll)

    xpart, cpart = at_row(z, 1 - xh, k), at_row(z, xh, 1 - k)
    lpart = at_col(y, 1 - xl)

    barrier = pltpu.get_barrier_semaphore()
    near = [xpart, cpart, lpart]
    for d in (2, -2, 1, -1):
        near += [at_row(z + d, xh, k), at_col(y + d, xl)]
    for peer in near:
        pl.semaphore_signal(barrier, inc=1, device_id=peer, device_id_type=MESH)

    fetches = [
        pltpu.make_async_copy(src, dst, in_s.at[n])
        for n, (src, dst) in enumerate(
            ((pan, praw), (blk, hits), (anc, ebuf), (lnk.at[0], bb.at[kk, k]), (inv, low))
        )
    ]
    for fetch in fetches:
        fetch.start()

    first = (r * 16 + c) * 24
    b0 = first // BLOCK
    b1 = (first + 23) // BLOCK
    fetches[0].wait()
    fetches[1].wait()
    upper = lax.broadcasted_iota(jnp.int32, (24, 512), 0) < (b0 + 1) * BLOCK - first
    for s, pb in enumerate((pb0, pb1)):
        row = hits[s : s + 1, :]
        hit0 = jnp.max(jnp.where(row == b0, 1.0, 0.0), axis=1, keepdims=True)
        hit1 = jnp.max(jnp.where(row == b1, 1.0, 0.0), axis=1, keepdims=True)
        keep = jnp.where(upper, hit0, hit1)
        pb[kk, k] = jnp.where(keep > 0.5, praw[s], 0.0)

    pl.semaphore_wait(barrier, len(near))

    sends = []

    def remote(src, dst, ss, rs, to):
        return pltpu.make_async_remote_copy(
            src_ref=src, dst_ref=dst, send_sem=ss, recv_sem=rs, device_id=to, device_id_type=MESH
        )

    streams = (pb0, pb1, bb)
    place = (kk, z * 2 + 1 - xh)
    far = (1, -1)
    ring = {}

    def ag(q, name, block, to):
        n = len(ring)
        ref = streams[q].at[block, k]
        copy = remote(ref, ref, ag_s.at[n], ag_r.at[n], to)
        ring[q, name] = copy
        sends.append(copy)
        copy.start()

    def across(q):
        ag(q, "x", kk, xpart)

    def crossed(q):
        ring[q, "x"].wait_recv()

    def level1(q, line):
        for d in (2, -2, 1, -1):
            ag(q, f"{line}{d}", place[line], at_row(z + d, xh, k))
        ag(q, f"c{line}", place[line], cpart)

    def block_from(d, line):
        return wrap(z - d) * 2 + (xh if line == 0 else 1 - xh)

    def level2(q, line):
        for g in (far[line], -far[line]):
            ring[q, f"{line}{2 * g}"].wait_recv()
            block = block_from(2 * g, line)
            if g == far[line]:
                ag(q, f"{line}{4 * g}", block, at_row(z + 2 * g, xh, k))
            ag(q, f"{line}{3 * g}", block, at_row(z + g, xh, k))
            ag(q, f"c{line}{2 * g}", block, cpart)

    def handed(q, line, distances):
        for d in distances:
            ring[q, f"{line}{d}"].wait_recv()
            ag(q, f"c{line}{d}", block_from(d, line), cpart)

    def ones(q):
        handed(q, 0, (1, -1))
        handed(q, 1, (1, -1))

    def lasts(q, line):
        handed(q, line, (3 * far[line], -3 * far[line], 4 * far[line]))

    def close_stream(q):
        for (stream, name), copy in list(ring.items()):
            if stream == q and name[0] == "c":
                copy.wait_recv()

    rsn = []

    def rs(src, dst, to):
        n = len(rsn)
        copy = remote(src, dst, rs_s.at[n], rs_r.at[n], to)
        rsn.append(copy)
        sends.append(copy)
        copy.start()
        return copy

    def product(pb, out):
        def step(n, _):
            at = pl.ds(pl.multiple_of(n * 256, 256), 256)
            ph, plo = halves_of(pb[:, :, :, at].reshape(768, 256))
            out[:, :, :, at] = dot3(ehi[...], elo[...], ph, plo).reshape(8, 2, 24, 256)
            return 0

        lax.fori_loop(0, 2, step, 0)

    def yy(d):
        return wrap(y + d)

    folded = (f0, f1)
    tree = {}

    def exchange(s):
        g = far[s]
        for d in (4 * g, 3 * g, -3 * g, 2 * g, -2 * g, g, -g, 0):
            tree[s, "x", d] = rs(folded[s].at[yy(d), 1 - xl], xa.at[s, yy(d)], lpart)

    def value(s, d):
        tree[s, "x", d].wait_recv()
        return folded[s][yy(d), xl] + xa[s, yy(d)]

    def arrive(s, d):
        tree[s, d].wait_recv()
        return rbuf[s, slots.index(d * far[s])]

    slots = [4, 3, -3, 2, -2, 1, -1]

    def pass_on(s, d, part, to):
        n = slots.index(d * far[s])
        sbuf[s, n] = part
        tree[s, d] = rs(sbuf.at[s, n], rbuf.at[s, n], at_col(y + to, xl))

    def sum_a(s):
        g = far[s]
        pass_on(s, 4 * g, value(s, 4 * g), 2 * g)
        pass_on(s, 3 * g, value(s, 3 * g), g)
        pass_on(s, -3 * g, value(s, -3 * g), -g)

    def sum_b(s):
        g = far[s]
        part = value(s, 2 * g) + arrive(s, 3 * g)
        pass_on(s, 2 * g, part + arrive(s, 4 * g), 2 * g)
        pass_on(s, -2 * g, value(s, -2 * g) + arrive(s, -3 * g), -2 * g)

    def sum_c(s):
        g = far[s]
        pass_on(s, g, value(s, g), g)
        pass_on(s, -g, value(s, -g), -g)

    def summed(s):
        total = value(s, 0)
        for d in (1, -1, -2, 2):
            total = total + arrive(s, d * far[s])
        return total

    across(0)
    level1(0, 0)
    across(1)
    fetches[3].wait()
    across(2)
    fetches[2].wait()
    for i in range(6):
        at = slice(i * 128, (i + 1) * 128)
        h, l = halves_of(ebuf[at, :].T)
        ehi[:, at] = h
        elo[:, at] = l
    crossed(0)
    level1(0, 1)
    level2(0, 0)
    level2(0, 1)
    level1(1, 0)
    crossed(1)
    level1(1, 1)
    ones(0)
    lasts(0, 0)
    lasts(0, 1)
    close_stream(0)
    product(pb0, f0)
    exchange(0)
    level2(1, 0)
    level2(1, 1)
    crossed(2)
    level1(2, 0)
    level1(2, 1)
    sum_a(0)
    ones(1)
    lasts(1, 0)
    lasts(1, 1)
    close_stream(1)
    product(pb1, f1)
    exchange(1)
    sum_b(0)
    level2(2, 0)
    level2(2, 1)
    sum_c(0)
    for g in range(3):
        at = slice(g * 128, (g + 1) * 128)
        rows = slice(g * 8, g * 8 + 8)
        for s, pb in enumerate((pb0, pb1)):
            h, l = halves_of(pb[:, pl.ds(k, 1), rows, :].reshape(128, 512))
            prh[at, s * 512 : s * 512 + 512] = h
            prl[at, s * 512 : s * 512 + 512] = l
    sum_a(1)
    ones(2)
    lasts(2, 0)
    lasts(2, 1)
    sum_b(1)
    sum_c(1)
    close_stream(2)
    for g in range(4):
        at = slice(g * 128, (g + 1) * 128)
        h, l = halves_of(bb[g * 4 : g * 4 + 4].reshape(128, 512))
        bhi[at, :] = h
        blo[at, :] = l

    c0 = -summed(0)
    h, l = halves_of(c0)
    carried = dot3(h, l, bhi[...], blo[...])
    cols[0] = c0

    def owner(chip):
        zc, hc = chip // 2, chip % 2
        return lax.rem(16 - zc - y, 8) * 2 + jnp.where(hc == xl, 0, 1)

    def packed(value, q):
        at = slice((q // 4) * 128, (q // 4) * 128 + 128)
        o = (q % 4) * 32
        v = [turned(value[g * 8 : g * 8 + 8, at], g * 32 - o) for g in range(3)]
        return jnp.where(lane < 32, v[0], jnp.where(lane < 64, v[1], v[2]))

    part = owner(kk)

    def settle(buf, count, sem):
        pltpu.make_async_copy(buf.at[pl.ds(0, count)], buf.at[pl.ds(0, count)], sem).wait()

    def spread(send, recv, n):
        def step(i, _):
            to = lax.rem(kk + i, 16)
            remote(send.at[owner(to)], recv.at[kk], ex_s.at[n], ex_r.at[n], (to * 2 + k, c)).start()
            return 0

        lax.fori_loop(1, 16, step, 0)
        recv[kk] = send[part]

    for q in range(16):
        s0send[q, 0] = packed(c0, q)
        s0send[q, 1] = packed(carried, q)
    spread(s0send, s0buf, 1)

    for g in range(3):
        at = slice(g * 128, (g + 1) * 128)
        rh, rl = halves_of(dot3(prh[at, 0:512], prl[at, 0:512], bhi[...], blo[...]))
        prh[at, 1024:1536] = rh
        prl[at, 1024:1536] = rl

    c1 = -(summed(1) + carried)
    for q in range(16):
        s1send[q] = packed(c1, q)
    spread(s1send, s1buf, 2)
    cols[1] = c1

    fetches[4].wait()
    tri = lax.broadcasted_iota(jnp.int32, (16, 512), 1) <= r * 16 + lax.broadcasted_iota(jnp.int32, (16, 512), 0)
    l0 = jnp.where(tri, low[0], 0.0)
    l1 = jnp.where(tri, low[1], 0.0)
    h, l = halves_of(l0)
    gsend[0:16, :] = l0
    gsend[16:32, :] = l1
    gsend[32:48, :] = dot3(h, l, bhi[...], blo[...])
    chunk = gsend[:, pl.ds(pl.multiple_of((c // 4) * 128, 128), 128)]
    off = lax.rem(c, 4) * 32
    to0 = pltpu.roll(chunk, lax.rem(128 - off, 128), 1)
    to1 = pltpu.roll(chunk, lax.rem(160 - off, 128), 1)
    row = lax.broadcasted_iota(jnp.int32, (48, 128), 0)
    wide = jnp.where(row < 16, jnp.where(lane < 32, to0, 0.0), jnp.where((lane >= 32) & (lane < 64), to1, 0.0))
    wide = wide + pltpu.roll(wide, 64, 1)
    zeros = jnp.zeros((80, 512), F32)
    uh, ul = halves_of(jnp.concatenate([gsend[...], zeros], axis=0).T)
    wh, wl = halves_of(jnp.concatenate([wide, zeros[:, 0:128]], axis=0))
    gpart = dot3(uh, ul, wh, wl).reshape(32, 2, 8, 128)
    gbuf[0] = jnp.where(lane < 64, gpart[:, 0], gpart[:, 1])

    def send_g(i, _):
        to = lax.rem(r + i, 32)
        remote(gbuf.at[0, to], gbuf.at[1, r], ex_s.at[0], ex_r.at[0], (to, c)).start()
        return 0

    lax.fori_loop(1, 32, send_g, 0)
    gbuf[1, r] = gbuf[0, r]

    def left_of(tiles):
        t = tiles.reshape(128, 128).T
        return jnp.concatenate([t[0:32], t[32:64], t[64:96]], axis=1)

    slot = c * 2 + k

    def scatter(send, recv, n, start, target, inside):
        def step(i, _):
            to = lax.rem(start + i, 32)
            remote(send.at[to], recv.at[slot], ex_s.at[n], ex_r.at[n], target(to)).start()
            return 0

        lax.fori_loop(1, 32, step, 0)

        @pl.when(inside)
        def _():
            recv[slot] = send[start]

        @pl.when(jnp.logical_not(inside))
        def _():
            remote(send.at[start], recv.at[slot], ex_s.at[n], ex_r.at[n], target(start)).start()

    def settle_scatter(buf, sem, inside):
        @pl.when(inside)
        def _():
            settle(buf, 31, sem)

        @pl.when(jnp.logical_not(inside))
        def _():
            settle(buf, 32, sem)

    settle(s0buf, 15, ex_r.at[1])
    h, l = halves_of(jnp.concatenate([left_of(s0buf[:, 0]), left_of(s0buf[:, 1])], axis=0))
    out = dot3(h, l, prh[...], prl[...])
    d0 = -out[0:32, 0:512]
    kept = out[32:64, 1024:1536]
    tt = out[32:64, 512:1024].reshape(2, 2, 8, 512)
    for q in range(16):
        at = slice((q // 4) * 128, (q // 4) * 128 + 128)
        o = (q % 4) * 32
        for half in range(2):
            upper_rows = turned(tt[half, 0, :, at], 32 - o)
            lower_rows = turned(tt[half, 1, :, at], 96 - o)
            tsend[q * 2 + half] = jnp.where(
                lane >= 96, lower_rows, jnp.where((lane >= 32) & (lane < 64), upper_rows, 0.0)
            )
    t_inside = part == kk
    scatter(tsend, tbuf, 3, slot, lambda to: (part * 2 + lax.rem(to, 2), to // 2), t_inside)

    settle(s1buf, 15, ex_r.at[2])
    h, l = halves_of(left_of(s1buf[...]))
    d1 = -(dot3(h, l, prh[:, 512:1024], prl[:, 512:1024]) + kept)
    dt = jnp.concatenate([d0, d1, d0, d1], axis=0).T.reshape(32, 2, 8, 128)
    dsend[...] = jnp.where(lane < 64, dt[:, 0], dt[:, 1])
    d_inside = part == c
    scatter(dsend, dbuf, 4, r, lambda to: (to, part), d_inside)

    settle(gbuf.at[1], 31, ex_r.at[0])
    total = jnp.sum(gbuf[1], axis=0)
    settle_scatter(tbuf, ex_r.at[3], t_inside)
    total = total + jnp.sum(tbuf[...], axis=0)
    settle_scatter(dbuf, ex_r.at[4], d_inside)
    total = total + jnp.sum(dbuf[...], axis=0)
    diag[0, 0:8, :] = total[:, 0:32]
    diag[1, 0:8, :] = turned(total, 96)[:, 0:32]
    diag[0, 8:16, :] = turned(total, 64)[:, 0:32]
    diag[1, 8:16, :] = turned(total, 32)[:, 0:32]

    settle(gbuf.at[1], 31, ex_s.at[0])
    settle(s0buf, 15, ex_s.at[1])
    settle(s1buf, 15, ex_s.at[2])
    settle_scatter(tbuf, ex_s.at[3], t_inside)
    settle_scatter(dbuf, ex_s.at[4], d_inside)
    for copy in sends:
        copy.wait_send()


def body(ancestor, panels, link_panels, diag_inverse, blocks):
    vmem = pl.BlockSpec(memory_space=pltpu.VMEM)
    there = pl.BlockSpec(memory_space=pl.ANY)
    dma = pltpu.SemaphoreType.DMA
    return pl.pallas_call(
        kernel,
        out_shape=(
            jax.ShapeDtypeStruct((2, 24, 512), F32),
            jax.ShapeDtypeStruct((2, 16, 32), F32),
        ),
        in_specs=[there] * 5,
        out_specs=(vmem, vmem),
        scratch_shapes=[
            pltpu.VMEM((16, 2, 24, 512), F32),
            pltpu.VMEM((16, 2, 24, 512), F32),
            pltpu.VMEM((16, 2, 16, 512), F32),
            pltpu.VMEM((2, 24, 512), F32),
            pltpu.VMEM((2, 16, 512), F32),
            pltpu.VMEM((2, 48), jnp.int32),
            pltpu.VMEM((768, 384), F32),
            pltpu.VMEM((384, 768), BF16),
            pltpu.VMEM((384, 768), BF16),
            pltpu.VMEM((8, 2, 24, 512), F32),
            pltpu.VMEM((8, 2, 24, 512), F32),
            pltpu.VMEM((2, 8, 24, 512), F32),
            pltpu.VMEM((2, 7, 24, 512), F32),
            pltpu.VMEM((2, 7, 24, 512), F32),
            pltpu.VMEM((512, 512), BF16),
            pltpu.VMEM((512, 512), BF16),
            pltpu.VMEM((384, 1536), BF16),
            pltpu.VMEM((384, 1536), BF16),
            pltpu.VMEM((16, 2, 8, 128), F32),
            pltpu.VMEM((16, 2, 8, 128), F32),
            pltpu.VMEM((16, 8, 128), F32),
            pltpu.VMEM((16, 8, 128), F32),
            pltpu.VMEM((32, 8, 128), F32),
            pltpu.VMEM((32, 8, 128), F32),
            pltpu.VMEM((32, 8, 128), F32),
            pltpu.VMEM((32, 8, 128), F32),
            pltpu.VMEM((48, 512), F32),
            pltpu.VMEM((2, 32, 8, 128), F32),
            dma((5,)),
            dma((93,)),
            dma((93,)),
            dma((30,)),
            dma((30,)),
            dma((5,)),
            dma((5,)),
        ],
        compiler_params=pltpu.CompilerParams(
            collective_id=0, has_side_effects=True
        ),
    )(
        ancestor.reshape(ancestor.shape[0] * ancestor.shape[1], ancestor.shape[2]),
        panels,
        link_panels,
        diag_inverse,
        blocks,
    )


def solution(mesh):
    return jax.shard_map(
        body,
        mesh=mesh,
        in_specs=(
            P(None, "col", "row"),
            P(None, ("row", "col"), None),
            P(None, "row", None),
            P(None, "row", None),
            P(),
        ),
        out_specs=(P(None, ("row", "col"), None), P(None, "row", "col")),
        check_vma=False,
    )
```

```python
import jax
import jax.numpy as jnp
from jax import lax
from jax.experimental import pallas as pl
from jax.experimental.pallas import tpu as pltpu
from jax.sharding import PartitionSpec as P

BLOCK = 128
F32 = jnp.float32
BF16 = jnp.bfloat16
MESH = pl.DeviceIdType.MESH


def halves_of(value):
    high = value.astype(BF16)
    return high, (value - high.astype(F32)).astype(BF16)


def dot(left, right):
    return jnp.dot(left, right, preferred_element_type=F32)


def dot3(lh, ll, rh, rl):
    return dot(lh, rh) + (dot(lh, rl) + dot(ll, rh))


def thin(lh, ll, rh, rl):
    rows = lh.shape[0]
    both = dot(jnp.concatenate([lh, ll], axis=0), rh)
    return both[0:rows] + (both[rows:] + dot(lh, rl))


def turned(value, shift):
    shift = shift % 128
    return value if shift == 0 else pltpu.roll(value, shift, 1)


def kernel(
    anc, pan, lnk, inv, blk, cols, diag,
    pb0, pb1, bb, praw, low, hits, ebuf, ehi, elo, f0, f1, xa, sbuf, rbuf,
    bhi, blo, prh, prl, s0send, s0buf, s1send, s1buf, dsend, dbuf, tsend, tbuf, gsend, gbuf,
    in_s, ag_s, ag_r, rs_s, rs_r, ex_s, ex_r,
):
    r = lax.axis_index("row")
    c = lax.axis_index("col")
    z, xh, k = r // 4, (r // 2) % 2, r % 2
    y, xl = c // 2, c % 2
    kk = r // 2
    lane = lax.broadcasted_iota(jnp.int32, (1, 128), 1)

    def wrap(i):
        return lax.rem(i + 8, 8)

    def at_row(zz, hh, co):
        return (wrap(zz) * 4 + hh * 2 + co, c)

    def at_col(yy, ll):
        return (r, wrap(yy) * 2 + ll)

    xpart, cpart = at_row(z, 1 - xh, k), at_row(z, xh, 1 - k)
    lpart = at_col(y, 1 - xl)

    barrier = pltpu.get_barrier_semaphore()
    near = [xpart, cpart, lpart]
    for d in (2, -2, 1, -1):
        near += [at_row(z + d, xh, k), at_col(y + d, xl)]
    for peer in near:
        pl.semaphore_signal(barrier, inc=1, device_id=peer, device_id_type=MESH)

    fetches = [
        pltpu.make_async_copy(src, dst, in_s.at[n])
        for n, (src, dst) in enumerate(
            ((pan, praw), (blk, hits), (anc, ebuf), (lnk.at[0], bb.at[kk, k]), (inv, low))
        )
    ]
    for fetch in fetches:
        fetch.start()

    first = (r * 16 + c) * 24
    b0 = first // BLOCK
    b1 = (first + 23) // BLOCK
    fetches[0].wait()
    fetches[1].wait()
    upper = lax.broadcasted_iota(jnp.int32, (24, 512), 0) < (b0 + 1) * BLOCK - first
    for s, pb in enumerate((pb0, pb1)):
        row = hits[s : s + 1, :]
        hit0 = jnp.max(jnp.where(row == b0, 1.0, 0.0), axis=1, keepdims=True)
        hit1 = jnp.max(jnp.where(row == b1, 1.0, 0.0), axis=1, keepdims=True)
        keep = jnp.where(upper, hit0, hit1)
        pb[kk, k] = jnp.where(keep > 0.5, praw[s], 0.0)

    pl.semaphore_wait(barrier, len(near))

    sends = []

    def remote(src, dst, ss, rs, to):
        return pltpu.make_async_remote_copy(
            src_ref=src, dst_ref=dst, send_sem=ss, recv_sem=rs, device_id=to, device_id_type=MESH
        )

    streams = (pb0, pb1, bb)
    place = (kk, z * 2 + 1 - xh)
    far = (1, -1)
    ring = {}

    def ag(q, name, block, to):
        n = len(ring)
        ref = streams[q].at[block, k]
        copy = remote(ref, ref, ag_s.at[n], ag_r.at[n], to)
        ring[q, name] = copy
        sends.append(copy)
        copy.start()

    def across(q):
        ag(q, "x", kk, xpart)

    def crossed(q):
        ring[q, "x"].wait_recv()

    def level1(q, line):
        for d in (2, -2, 1, -1):
            ag(q, f"{line}{d}", place[line], at_row(z + d, xh, k))
        ag(q, f"c{line}", place[line], cpart)

    def block_from(d, line):
        return wrap(z - d) * 2 + (xh if line == 0 else 1 - xh)

    def level2(q, line):
        for g in (far[line], -far[line]):
            ring[q, f"{line}{2 * g}"].wait_recv()
            block = block_from(2 * g, line)
            if g == far[line]:
                ag(q, f"{line}{4 * g}", block, at_row(z + 2 * g, xh, k))
            ag(q, f"{line}{3 * g}", block, at_row(z + g, xh, k))
            ag(q, f"c{line}{2 * g}", block, cpart)

    def handed(q, line, distances):
        for d in distances:
            ring[q, f"{line}{d}"].wait_recv()
            ag(q, f"c{line}{d}", block_from(d, line), cpart)

    def ones(q):
        handed(q, 0, (1, -1))
        handed(q, 1, (1, -1))

    def lasts(q, line):
        handed(q, line, (3 * far[line], -3 * far[line], 4 * far[line]))

    def close_stream(q):
        for (stream, name), copy in list(ring.items()):
            if stream == q and name[0] == "c":
                copy.wait_recv()

    rsn = []

    def rs(src, dst, to):
        n = len(rsn)
        copy = remote(src, dst, rs_s.at[n], rs_r.at[n], to)
        rsn.append(copy)
        sends.append(copy)
        copy.start()
        return copy

    def product(pb, out):
        def step(n, _):
            at = pl.ds(pl.multiple_of(n * 256, 256), 256)
            ph, plo = halves_of(pb[:, :, :, at].reshape(768, 256))
            out[:, :, :, at] = dot3(ehi[...], elo[...], ph, plo).reshape(8, 2, 24, 256)
            return 0

        lax.fori_loop(0, 2, step, 0)

    def yy(d):
        return wrap(y + d)

    folded = (f0, f1)
    tree = {}

    def exchange(s):
        g = far[s]
        for d in (4 * g, 3 * g, -3 * g, 2 * g, -2 * g, g, -g, 0):
            tree[s, "x", d] = rs(folded[s].at[yy(d), 1 - xl], xa.at[s, yy(d)], lpart)

    def value(s, d):
        tree[s, "x", d].wait_recv()
        return folded[s][yy(d), xl] + xa[s, yy(d)]

    def arrive(s, d):
        tree[s, d].wait_recv()
        return rbuf[s, slots.index(d * far[s])]

    slots = [4, 3, -3, 2, -2, 1, -1]

    def pass_on(s, d, part, to):
        n = slots.index(d * far[s])
        sbuf[s, n] = part
        tree[s, d] = rs(sbuf.at[s, n], rbuf.at[s, n], at_col(y + to, xl))

    def sum_a(s):
        g = far[s]
        pass_on(s, 4 * g, value(s, 4 * g), 2 * g)
        pass_on(s, 3 * g, value(s, 3 * g), g)
        pass_on(s, -3 * g, value(s, -3 * g), -g)

    def sum_b(s):
        g = far[s]
        part = value(s, 2 * g) + arrive(s, 3 * g)
        pass_on(s, 2 * g, part + arrive(s, 4 * g), 2 * g)
        pass_on(s, -2 * g, value(s, -2 * g) + arrive(s, -3 * g), -2 * g)

    def sum_c(s):
        g = far[s]
        pass_on(s, g, value(s, g), g)
        pass_on(s, -g, value(s, -g), -g)

    def summed(s):
        total = value(s, 0)
        for d in (1, -1, -2, 2):
            total = total + arrive(s, d * far[s])
        return total

    across(0)
    level1(0, 0)
    across(1)
    fetches[3].wait()
    across(2)
    fetches[2].wait()
    for i in range(6):
        at = slice(i * 128, (i + 1) * 128)
        h, l = halves_of(ebuf[at, :].T)
        ehi[:, at] = h
        elo[:, at] = l
    crossed(0)
    level1(0, 1)
    level2(0, 0)
    level2(0, 1)
    level1(1, 0)
    crossed(1)
    level1(1, 1)
    ones(0)
    lasts(0, 0)
    lasts(0, 1)
    close_stream(0)
    product(pb0, f0)
    exchange(0)
    level2(1, 0)
    level2(1, 1)
    crossed(2)
    level1(2, 0)
    level1(2, 1)
    sum_a(0)
    ones(1)
    lasts(1, 0)
    lasts(1, 1)
    close_stream(1)
    product(pb1, f1)
    exchange(1)
    sum_b(0)
    level2(2, 0)
    level2(2, 1)
    sum_c(0)
    sum_a(1)
    for g in range(3):
        at = slice(g * 128, (g + 1) * 128)
        rows = slice(g * 8, g * 8 + 8)
        for s, pb in enumerate((pb0, pb1)):
            h, l = halves_of(pb[:, pl.ds(k, 1), rows, :].reshape(128, 512))
            prh[at, s * 512 : s * 512 + 512] = h
            prl[at, s * 512 : s * 512 + 512] = l
    ones(2)
    lasts(2, 0)
    lasts(2, 1)
    sum_b(1)
    sum_c(1)
    close_stream(2)
    for g in range(4):
        at = slice(g * 128, (g + 1) * 128)
        h, l = halves_of(bb[g * 4 : g * 4 + 4].reshape(128, 512))
        bhi[at, :] = h
        blo[at, :] = l

    c0 = -summed(0)
    h, l = halves_of(c0)
    carried = dot3(h, l, bhi[...], blo[...])
    cols[0] = c0

    def owner(chip):
        zc, hc = chip // 2, chip % 2
        return lax.rem(16 - zc - y, 8) * 2 + jnp.where(hc == xl, 0, 1)

    def packed(value, q):
        at = slice((q // 4) * 128, (q // 4) * 128 + 128)
        o = (q % 4) * 32
        v = [turned(value[g * 8 : g * 8 + 8, at], g * 32 - o) for g in range(3)]
        return jnp.where(lane < 32, v[0], jnp.where(lane < 64, v[1], v[2]))

    part = owner(kk)

    def settle(buf, count, sem):
        pltpu.make_async_copy(buf.at[pl.ds(0, count)], buf.at[pl.ds(0, count)], sem).wait()

    def spread(send, recv, n):
        def step(i, _):
            to = lax.rem(kk + i, 16)
            remote(send.at[owner(to)], recv.at[kk], ex_s.at[n], ex_r.at[n], (to * 2 + k, c)).start()
            return 0

        lax.fori_loop(1, 16, step, 0)
        recv[kk] = send[part]

    for q in range(16):
        s0send[q, 0] = packed(c0, q)
        s0send[q, 1] = packed(carried, q)
    spread(s0send, s0buf, 1)

    c1 = -(summed(1) + carried)
    for q in range(16):
        s1send[q] = packed(c1, q)
    spread(s1send, s1buf, 2)
    cols[1] = c1

    fetches[4].wait()
    tri = lax.broadcasted_iota(jnp.int32, (16, 512), 1) <= r * 16 + lax.broadcasted_iota(jnp.int32, (16, 512), 0)
    l0 = jnp.where(tri, low[0], 0.0)
    l1 = jnp.where(tri, low[1], 0.0)
    h, l = halves_of(l0)
    gsend[0:16, :] = l0
    gsend[16:32, :] = l1
    gsend[32:48, :] = thin(h, l, bhi[...], blo[...])
    chunk = gsend[:, pl.ds(pl.multiple_of((c // 4) * 128, 128), 128)]
    off = lax.rem(c, 4) * 32
    to0 = pltpu.roll(chunk, lax.rem(128 - off, 128), 1)
    to1 = pltpu.roll(chunk, lax.rem(160 - off, 128), 1)
    row = lax.broadcasted_iota(jnp.int32, (48, 128), 0)
    wide = jnp.where(row < 16, jnp.where(lane < 32, to0, 0.0), jnp.where((lane >= 32) & (lane < 64), to1, 0.0))
    wide = wide + pltpu.roll(wide, 64, 1)
    zeros = jnp.zeros((80, 512), F32)
    uh, ul = halves_of(jnp.concatenate([gsend[...], zeros], axis=0).T)
    wh, wl = halves_of(jnp.concatenate([wide, zeros[:, 0:128]], axis=0))
    gpart = dot3(uh, ul, wh, wl).reshape(32, 2, 8, 128)
    gbuf[0] = jnp.where(lane < 64, gpart[:, 0], gpart[:, 1])

    def send_g(i, _):
        to = lax.rem(r + i, 32)
        remote(gbuf.at[0, to], gbuf.at[1, r], ex_s.at[0], ex_r.at[0], (to, c)).start()
        return 0

    lax.fori_loop(1, 32, send_g, 0)
    gbuf[1, r] = gbuf[0, r]

    for g in range(3):
        at = slice(g * 128, (g + 1) * 128)
        rh, rl = halves_of(dot3(prh[at, 0:512], prl[at, 0:512], bhi[...], blo[...]))
        prh[at, 1024:1536] = rh
        prl[at, 1024:1536] = rl

    def left_of(tiles):
        t = tiles.reshape(128, 128).T
        return jnp.concatenate([t[0:32], t[32:64], t[64:96]], axis=1)

    slot = c * 2 + k

    def scatter(send, recv, n, start, target, inside):
        def step(i, _):
            to = lax.rem(start + i, 32)
            remote(send.at[to], recv.at[slot], ex_s.at[n], ex_r.at[n], target(to)).start()
            return 0

        lax.fori_loop(1, 32, step, 0)

        @pl.when(inside)
        def _():
            recv[slot] = send[start]

        @pl.when(jnp.logical_not(inside))
        def _():
            remote(send.at[start], recv.at[slot], ex_s.at[n], ex_r.at[n], target(start)).start()

    def settle_scatter(buf, sem, inside):
        @pl.when(inside)
        def _():
            settle(buf, 31, sem)

        @pl.when(jnp.logical_not(inside))
        def _():
            settle(buf, 32, sem)

    settle(s0buf, 15, ex_r.at[1])
    h, l = halves_of(jnp.concatenate([left_of(s0buf[:, 0]), left_of(s0buf[:, 1])], axis=0))
    out = thin(h, l, prh[...], prl[...])
    d0 = -out[0:32, 0:512]
    kept = out[32:64, 1024:1536]
    tt = out[32:64, 512:1024].reshape(2, 2, 8, 512)
    for q in range(16):
        at = slice((q // 4) * 128, (q // 4) * 128 + 128)
        o = (q % 4) * 32
        for half in range(2):
            upper_rows = turned(tt[half, 0, :, at], 32 - o)
            lower_rows = turned(tt[half, 1, :, at], 96 - o)
            tsend[q * 2 + half] = jnp.where(
                lane >= 96, lower_rows, jnp.where((lane >= 32) & (lane < 64), upper_rows, 0.0)
            )
    t_inside = part == kk
    scatter(tsend, tbuf, 3, slot, lambda to: (part * 2 + lax.rem(to, 2), to // 2), t_inside)

    settle(s1buf, 15, ex_r.at[2])
    h, l = halves_of(left_of(s1buf[...]))
    d1 = -(thin(h, l, prh[:, 512:1024], prl[:, 512:1024]) + kept)
    dt = jnp.concatenate([d0, d1, d0, d1], axis=0).T.reshape(32, 2, 8, 128)
    dsend[...] = jnp.where(lane < 64, dt[:, 0], dt[:, 1])
    d_inside = part == c
    scatter(dsend, dbuf, 4, r, lambda to: (to, part), d_inside)

    settle(gbuf.at[1], 31, ex_r.at[0])
    total = jnp.sum(gbuf[1], axis=0)
    settle_scatter(tbuf, ex_r.at[3], t_inside)
    total = total + jnp.sum(tbuf[...], axis=0)
    settle_scatter(dbuf, ex_r.at[4], d_inside)
    total = total + jnp.sum(dbuf[...], axis=0)
    diag[0, 0:8, :] = total[:, 0:32]
    diag[1, 0:8, :] = turned(total, 96)[:, 0:32]
    diag[0, 8:16, :] = turned(total, 64)[:, 0:32]
    diag[1, 8:16, :] = turned(total, 32)[:, 0:32]

    settle(gbuf.at[1], 31, ex_s.at[0])
    settle(s0buf, 15, ex_s.at[1])
    settle(s1buf, 15, ex_s.at[2])
    settle_scatter(tbuf, ex_s.at[3], t_inside)
    settle_scatter(dbuf, ex_s.at[4], d_inside)
    for copy in sends:
        copy.wait_send()


def body(ancestor, panels, link_panels, diag_inverse, blocks):
    vmem = pl.BlockSpec(memory_space=pltpu.VMEM)
    there = pl.BlockSpec(memory_space=pl.ANY)
    dma = pltpu.SemaphoreType.DMA
    return pl.pallas_call(
        kernel,
        out_shape=(
            jax.ShapeDtypeStruct((2, 24, 512), F32),
            jax.ShapeDtypeStruct((2, 16, 32), F32),
        ),
        in_specs=[there] * 5,
        out_specs=(vmem, vmem),
        scratch_shapes=[
            pltpu.VMEM((16, 2, 24, 512), F32),
            pltpu.VMEM((16, 2, 24, 512), F32),
            pltpu.VMEM((16, 2, 16, 512), F32),
            pltpu.VMEM((2, 24, 512), F32),
            pltpu.VMEM((2, 16, 512), F32),
            pltpu.VMEM((2, 48), jnp.int32),
            pltpu.VMEM((768, 384), F32),
            pltpu.VMEM((384, 768), BF16),
            pltpu.VMEM((384, 768), BF16),
            pltpu.VMEM((8, 2, 24, 512), F32),
            pltpu.VMEM((8, 2, 24, 512), F32),
            pltpu.VMEM((2, 8, 24, 512), F32),
            pltpu.VMEM((2, 7, 24, 512), F32),
            pltpu.VMEM((2, 7, 24, 512), F32),
            pltpu.VMEM((512, 512), BF16),
            pltpu.VMEM((512, 512), BF16),
            pltpu.VMEM((384, 1536), BF16),
            pltpu.VMEM((384, 1536), BF16),
            pltpu.VMEM((16, 2, 8, 128), F32),
            pltpu.VMEM((16, 2, 8, 128), F32),
            pltpu.VMEM((16, 8, 128), F32),
            pltpu.VMEM((16, 8, 128), F32),
            pltpu.VMEM((32, 8, 128), F32),
            pltpu.VMEM((32, 8, 128), F32),
            pltpu.VMEM((32, 8, 128), F32),
            pltpu.VMEM((32, 8, 128), F32),
            pltpu.VMEM((48, 512), F32),
            pltpu.VMEM((2, 32, 8, 128), F32),
            dma((5,)),
            dma((93,)),
            dma((93,)),
            dma((30,)),
            dma((30,)),
            dma((5,)),
            dma((5,)),
        ],
        compiler_params=pltpu.CompilerParams(
            collective_id=0, has_side_effects=True, vmem_limit_bytes=56300000
        ),
    )(
        *(
            pltpu.with_memory_space_constraint(value, pltpu.HBM)
            for value in (
                ancestor.reshape(ancestor.shape[0] * ancestor.shape[1], ancestor.shape[2]),
                panels,
                link_panels,
                diag_inverse,
                blocks,
            )
        )
    )


def solution(mesh):
    return jax.shard_map(
        body,
        mesh=mesh,
        in_specs=(
            P(None, "col", "row"),
            P(None, ("row", "col"), None),
            P(None, "row", None),
            P(None, "row", None),
            P(),
        ),
        out_specs=(P(None, ("row", "col"), None), P(None, "row", "col")),
        check_vma=False,
    )
```
